256 devices in a mesh: grp: 4 (over y), col: 64 (over x, z, core).
Axes of the slice: x: 4, y: 4, z: 8, core: 2. Of those that a mesh axis runs over, the one named last changes fastest.
Arguments:
- panels: bfloat16 [256, 4, 512, 512], P('col', None, 'grp'), may hold values from -1.296875 to 1.296875
- parent: float32 [256, 512, 512], P('col', 'grp'), may hold values from -6 to 6
- src_block: int32 [64, 40], P('col'), may hold values from 0 to 39, each once within a row
- dest_owner: int32 [2560, 1], P('col'), may hold values from 0 to 63; in each aligned block of 40 rows (0 to 39, 40 to 79, ...) no two rows name the same one
- target: int32 [2560], P('col'), may hold values from 0 to 3
- counts: int32 [64], P('col'), may hold values from 20 to 40, as said below
Outputs:
- assembled: float32 [256, 512, 512], P('col', 'grp')
The draws below stay inside these ranges and needn't reach their ends.
Inputs may be any that keep to these rules, and one draw needn't show every extreme that they name: `src_block`: each row of a column rank is a permutation of the 40 block pairs. `dest_owner`: among the 40 slots of one column rank at most 1 name the same owner. The live slots of a rank are its first counts[c]; some rank has all 40 live.
All inputs are finite; a program needn't handle non-finite values.
Results may differ from the reference program's by a relative error of at most 0.0026.
Values may be sent and summed in bfloat16 or wider, within the bound.
A program may use at most 128 MiB of HBM per device.

```python
import math
import jax
import jax.numpy as jnp
import numpy as np
from jax import lax

WIDTH = 512
BLOCK = 512
ROW_BLOCKS = 4
FRONTS = 4
TARGETS = 4
PAIRS = 10
SLOTS = 40
CAPACITY = 1
N_COL = 64


def draw_counts(key, part):
    values = jax.random.randint(key, (N_COL,), SLOTS // 2, SLOTS + 1).astype(jnp.int32)
    chosen = jax.random.randint(jax.random.fold_in(key, 7), (), 0, N_COL)
    return values.at[chosen].set(SLOTS)


def set_ends(drawn, own_key, least, high):
    index_at = [jax.random.randint(jax.random.fold_in(own_key, axis), (), 0, length) for axis, length in enumerate(drawn.shape)]
    widest = drawn.shape.index(max(drawn.shape))
    next_to = index_at[:widest] + [(index_at[widest] + 1) % drawn.shape[widest]] + index_at[widest + 1:]
    return drawn.at[tuple(index_at)].set(least).at[tuple(next_to)].set(high)


def level_of(stream_key, shape, cuts, low, top_value):
    def one(position, shards_of):
        steps = jax.random.uniform(jax.random.fold_in(jax.random.fold_in(stream_key, 6), position), (shards_of,), jnp.float32, low / len(cuts), top_value / len(cuts))
        return jnp.repeat(jnp.exp(steps), shape[position] // shards_of).reshape((-1,) + (1,) * (len(shape) - position - 1))

    factor_of = one(*cuts[0])
    for cut in cuts[1:]:
        factor_of = factor_of * one(*cut)
    return factor_of


def shared_out(stream_key, own, number, rows, amount, top, bound, slope):
    ranking = jax.random.permutation(stream_key, amount)
    crowded, common = load_shares(amount, rows * top, bound, slope, True), load_shares(amount, rows * top, bound, slope, False)
    places = jnp.arange(amount)

    def named(lengths, turn):
        used = int((lengths > 0).sum())
        fixed = max(1, used // 4)
        passed = fixed + (places - fixed + turn * (used - fixed)) % max(1, amount - fixed)
        return jnp.zeros((amount,), jnp.int32).at[ranking[jnp.where(places < fixed, places, passed)]].set(jnp.asarray(lengths, jnp.int32))

    lengths = jnp.where(number % 4 == 0, named(crowded, number // 4), named(common, number - number // 4 - 1))
    mixed = jax.random.permutation(jax.random.fold_in(own, 3), amount)
    giver, sink = mixed[0:amount // 2 * 2:2], mixed[1:amount // 2 * 2:2]
    slack = jnp.minimum(lengths[giver] - 1, bound - lengths[sink]) // 2
    slack = jnp.where((giver == ranking[0]) | (sink == ranking[0]) | (lengths[sink] == 0), 0, jnp.maximum(slack, 0))
    passed = jax.random.randint(jax.random.fold_in(own, 4), (amount // 2,), 0, 1 << 20) % (slack + 1)
    lengths = lengths.at[giver].add(-passed).at[sink].add(passed)
    members = jnp.searchsorted(jnp.cumsum(lengths), jnp.arange(rows * top), side="right").astype(jnp.int32)
    listing = members.reshape(top, rows).T
    listing = listing[jax.random.permutation(jax.random.fold_in(own, 1), rows)]
    turn = jax.random.randint(jax.random.fold_in(own, 2), (rows, 1), 0, top)
    return jnp.take_along_axis(listing, (jnp.arange(top)[None, :] + turn) % top, axis=1)


def load_shares(amount, total, most, skew, full):
    portions = [(1 << 20) // math.isqrt(rank ** skew) + 1 for rank in range(1, amount + 1)]
    largest = most if full else min(most, max(-(-total // amount), total * portions[0] // sum(portions)))
    least = 1 if total - largest >= amount - 1 else 0
    given, rest = [largest] + [least] * (amount - 1), total - largest - least * (amount - 1)
    while rest > 0:
        candidates = [i for i in range(1, amount) if given[i] < largest] or [i for i in range(1, amount) if given[i] < most]
        whole, remaining = sum([portions[i] for i in candidates]), rest
        for i in candidates:
            addition = min(most - given[i], max(1, remaining * portions[i] // whole), rest)
            given[i] = given[i] + addition
            rest = rest - addition
    return np.array(given)


def centred(stream_key, shape, spread, most, shards=(), kind=jnp.bfloat16):
    result = jax.random.normal(stream_key, shape, jnp.float32) * spread
    if len(shards) > 0:
        result = level_of(stream_key, shape, shards, -0.22, 0.18) * result
    return jnp.clip(result, min=-most, max=most).astype(kind)


def setup_inputs(seed: int = 0) -> dict:
    streams_of = jax.random.split(jax.random.key(seed), 7)
    panels = centred(streams_of[0], (N_COL * FRONTS, ROW_BLOCKS, BLOCK, WIDTH), 0.21, 1.296875, ((0, 64), (2, 4)))
    parent = centred(streams_of[1], (N_COL * TARGETS, BLOCK, BLOCK), 1.0, 6.0, ((0, 64), (1, 4)), jnp.float32)
    src_block = jax.vmap(lambda own: jax.random.permutation(own, SLOTS))(jax.random.split(streams_of[2], N_COL)).reshape((N_COL, SLOTS)).astype(jnp.int32)
    dest_owner_keys = jax.random.split(jax.random.fold_in(streams_of[3], 1), (N_COL * SLOTS) // SLOTS)
    dest_owner_turns = jax.random.permutation(jax.random.fold_in(streams_of[3], 3), (N_COL * SLOTS) // SLOTS)
    dest_owner = jax.vmap(lambda own, number: shared_out(jax.random.fold_in(streams_of[3], 2), own, number, SLOTS, N_COL, 1, CAPACITY, 2))(dest_owner_keys, dest_owner_turns).reshape((N_COL * SLOTS, 1))
    target = set_ends(jax.random.randint(streams_of[4], (N_COL * SLOTS,), 0, TARGETS), jax.random.fold_in(streams_of[4], 1), 0, TARGETS - 1).astype(jnp.int32)
    counts = draw_counts(jax.random.fold_in(streams_of[6], 71), 0)
    return dict(panels=panels, parent=parent, src_block=src_block, dest_owner=dest_owner, target=target, counts=counts)


def reference(panels, parent, src_block, dest_owner, target, counts):
    running = parent.astype(jnp.float32)
    slot_index = jnp.arange(SLOTS, dtype=jnp.int32)
    upper_table = jnp.asarray(np.array([a for a in range(ROW_BLOCKS) for b in range(a + 1)], np.int32))
    lower_table = jnp.asarray(np.array([b for a in range(ROW_BLOCKS) for b in range(a + 1)], np.int32))

    def add_device(column_rank, running):
        own_panels = lax.dynamic_slice_in_dim(panels, (column_rank * FRONTS).astype(jnp.int32), FRONTS, 0)
        flat_rows = own_panels.astype(jnp.float32).reshape(FRONTS * ROW_BLOCKS, BLOCK, WIDTH)
        combos = lax.dynamic_index_in_dim(src_block, column_rank, 0, keepdims=False)
        front_of = combos // PAIRS
        within = combos % PAIRS
        left_index = (front_of * ROW_BLOCKS + upper_table[within]).astype(jnp.int32)
        right_index = (front_of * ROW_BLOCKS + lower_table[within]).astype(jnp.int32)
        left_rows = flat_rows[left_index]
        right_rows = flat_rows[right_index]
        updates = jnp.einsum("srw,scw->src", left_rows, right_rows, precision=lax.Precision.HIGHEST)
        updates = updates.astype(jnp.bfloat16).astype(jnp.float32)
        limit = lax.dynamic_index_in_dim(counts, column_rank, 0, keepdims=False)
        is_live = slot_index < limit
        updates = jnp.where(is_live[:, None, None], updates, jnp.zeros_like(updates))
        start = (column_rank * SLOTS).astype(jnp.int32)
        owner_rank = lax.dynamic_slice_in_dim(dest_owner[:, 0], start, SLOTS, 0)
        block_target = lax.dynamic_slice_in_dim(target, start, SLOTS, 0)
        dest_rows = (owner_rank * TARGETS + block_target).astype(jnp.int32)
        return running.at[dest_rows].add(-updates)

    return lax.fori_loop(0, N_COL, add_device, running)
```

```python
import jax
import jax.numpy as jnp
import numpy as np
from jax import lax
from jax.experimental import pallas as pl
from jax.experimental.pallas import tpu as pltpu
from jax.sharding import PartitionSpec as P

MESH = pl.DeviceIdType.MESH
NX, NZ, NY = 4, 8, 4
CHUNKS = 8
HR = 32
LANES = 128
UPPER = np.array([a for a in range(4) for b in range(a + 1)], np.int32)
LOWER = np.array([b for a in range(4) for b in range(a + 1)], np.int32)


def assemble_kernel(
    tab, panels, lab, parent, out,
    u0, u1, u2, u3, d0, d1, d2, d3,
    sendb, rx1, rlab, zsp, zrp, zsm, zrm, x2s, x2r, fin, yra, yrb, yrc,
    y_ss, y_rs, l_ss, l_rs, x1_ss, x1_rs, z_ss, z_rs, x2_ss, x2_rs, f_ss, f_rs,
):
    ups, downs = (u0, u1, u2, u3), (d0, d1, d2, d3)
    y = lax.axis_index("grp")
    col = lax.axis_index("col")
    core = lax.rem(col, 2)
    z = lax.rem(col // 2, NZ)
    x = col // (2 * NZ)

    def dev(yy, xx, zz, cc):
        return (lax.rem(yy + NY, NY), (lax.rem(xx + NX, NX) * NZ + lax.rem(zz + NZ, NZ)) * 2 + cc)

    sib = dev(y, x, z, 1 - core)
    s_of = [1 - 2 * lax.rem(x + h, 2) for h in range(2)]
    partner = [(dev(y, x + s, z, core), dev(y, x + s, z, 1 - core)) for s in s_of]
    second = [dev(y, x - s, z, core) for s in s_of]
    z_up, z_dn = dev(y, x, z + 1, core), dev(y, x, z - 1, core)
    y_up, y_dn = dev(y + 1, x, z, core), dev(y - 1, x, z, core)

    barrier = pltpu.get_barrier_semaphore()
    peers = [sib, partner[0][0], partner[0][1], partner[1][0], partner[1][1], z_up, z_dn, y_up, y_dn]
    for peer in peers:
        pl.semaphore_signal(barrier, inc=1, device_id=peer, device_id_type=MESH)
    pl.semaphore_wait(barrier, len(peers))

    def rcopy(src, dst, ss, rs, who):
        return pltpu.make_async_remote_copy(
            src_ref=src, dst_ref=dst, send_sem=ss, recv_sem=rs, device_id=who, device_id_type=MESH
        )

    def y_copy(q, side):
        dst = (ups if side == 0 else downs)[q]
        return rcopy(panels.at[:, q * HR:(q + 1) * HR, :], dst, y_ss.at[q, side], y_rs.at[q, side],
                     y_dn if side == 0 else y_up)

    def x1_who(h, k):
        return (sib, partner[h][0], partner[h][1])[k]

    def lab_copy(h, k):
        return rcopy(lab.at[h, k + 1], rlab.at[h, k], l_ss.at[h, k], l_rs.at[h, k], x1_who(h, k))

    def x1_copy(c, h, k):
        return rcopy(sendb.at[c, h, k + 1], rx1.at[c, h, k], x1_ss.at[c, h, k], x1_rs.at[c, h, k], x1_who(h, k))

    def z_first(c, side):
        src, dst, who = ((zsp, zrp, z_up), (zsm, zrm, z_dn))[side]
        return rcopy(src.at[c, 0, side], dst.at[c, 0, side], z_ss.at[c, 0, side], z_rs.at[c, 0, side], who)

    def z_copy(c, s, side):
        src, dst, who = ((zsp, zrp, z_up), (zsm, zrm, z_dn))[side]
        return rcopy(src.at[c, s], dst.at[c, s], z_ss.at[c, s, side], z_rs.at[c, s, side], who)

    def x2_copy(c, h):
        return rcopy(x2s.at[c, h], x2r.at[c, h], x2_ss.at[c, h], x2_rs.at[c, h], second[h])

    def f_copy_a(q):
        return rcopy(fin.at[2 + q, 0], yra.at[q], f_ss.at[q, 0], f_rs.at[q, 0], y_up)

    def f_copy_b(q):
        return rcopy(fin.at[2 + q, 1], yrb.at[q], f_ss.at[q, 1], f_rs.at[q, 1], y_dn)

    def f_copy_c(q):
        return rcopy(fin.at[6 + q], yrc.at[q], f_ss.at[4 + q, 0], f_rs.at[4 + q, 0], y_dn)

    for h in range(2):
        for k in range(3):
            lab_copy(h, k).start()
    for q in range(4):
        for side in range(2):
            y_copy(q, side).start()

    def multiply(c, part, left, right):
        def one(j, carry):
            n = part * 16 + j
            xo, zo, co = n // 16, lax.rem(n // 2, NZ), lax.rem(n, 2)
            ia, ib = tab[2 * n], tab[2 * n + 1]
            block = lax.dot_general(
                left(ia), right(ib), (((1,), (1,)), ((), ())), preferred_element_type=jnp.float32
            ).astype(jnp.bfloat16)
            cc = lax.rem(co + core, 2)
            for h in range(2):
                e = lax.rem((xo - x) * s_of[h] + 9, 4)
                sendb[c, h, (e // 2) * 2 + cc, zo * 2 + lax.rem(e, 2)] = block[h * HR:(h + 1) * HR]
            return carry

        lax.fori_loop(0, 16, one, 0, unroll=4)

    def products(c, part):
        own = lambda i: panels[i]

        for k in range(2):
            @pl.when(c == k)
            def _():
                multiply(c, part, lambda i: panels[i, k * 64:(k + 1) * 64, :], own)

        for q in range(4):
            @pl.when(c == 2 + q)
            def _():
                @pl.when(part == 0)
                def _():
                    y_copy(q, 0).wait_recv()
                    y_copy(q, 1).wait_recv()

                multiply(c, part, lambda i: jnp.concatenate([ups[q][i], downs[q][i]], axis=0), own)

        for k in range(2):
            @pl.when(c == 6 + k)
            def _():
                multiply(
                    c, part,
                    lambda i: jnp.concatenate([downs[2 * k][i], downs[2 * k + 1][i]], axis=0),
                    lambda i: jnp.concatenate([u[i] for u in ups], axis=0),
                )

    def x1_send(c):
        for h in range(2):
            for k in range(3):
                x1_copy(c, h, k).start()

    def local_sum(c, h, d, i, base):
        rows = d * 2 + i
        flip = d * 2 + (1 - i)
        blocks = [sendb[c, h, 0, rows], rx1[c, h, 0, rows], rx1[c, h, 1, flip], rx1[c, h, 2, flip]]
        labels = [lab[h, 0, pl.ds(rows, 1), :], rlab[h, 0, pl.ds(rows, 1), :],
                  rlab[h, 1, pl.ds(flip, 1), :], rlab[h, 2, pl.ds(flip, 1), :]]
        blocks = [b.astype(jnp.float32) for b in blocks]
        labels = [jnp.broadcast_to(v, (HR, LANES)) for v in labels]
        sums = []
        for t in range(4):
            total = None if base is None else base[t]
            for b, v in zip(blocks, labels):
                term = jnp.where(v == t + 1, b, 0.0)
                total = term if total is None else total + term
            sums.append(total)
        return sums

    def merge(c, s, h, d, prev, dst):
        for i in range(2):
            base = None if prev is None else [prev[c, s - 1, h, i * 4 + t].astype(jnp.float32) for t in range(4)]
            for t, v in enumerate(local_sum(c, h, d, i, base)):
                dst[c, s, h, i * 4 + t] = v.astype(jnp.bfloat16)

    def z_step(c, s):
        dp, dm = lax.rem(z + 4 - s, NZ), lax.rem(z + 4 + s, NZ)

        @pl.when(s == 0)
        def _():
            @pl.when(c == 0)
            def _():
                for h in range(2):
                    for k in range(3):
                        lab_copy(h, k).wait_recv()
            for h in range(2):
                for k in range(3):
                    x1_copy(c, h, k).wait_recv()
            merge(c, s, 0, dp, None, zsp)
            z_first(c, 0).start()
            merge(c, s, 1, dm, None, zsm)
            z_first(c, 1).start()

        @pl.when(s == 1)
        def _():
            z_first(c, 0).wait_recv()
            merge(c, s, 0, dp, zrp, zsp)
            merge(c, s, 1, dp, None, zsp)
            z_copy(c, s, 0).start()
            z_first(c, 1).wait_recv()
            merge(c, s, 1, dm, zrm, zsm)
            merge(c, s, 0, dm, None, zsm)
            z_copy(c, s, 1).start()

        @pl.when(s >= 2)
        def _():
            z_copy(c, s - 1, 0).wait_recv()
            for h in range(2):
                merge(c, s, h, dp, zrp, zsp)
            z_copy(c, s, 0).start()
            z_copy(c, s - 1, 1).wait_recv()
            for h in range(2):
                merge(c, s, h, dm, zrm, zsm)
            z_copy(c, s, 1).start()

    def z_last(c):
        z_copy(c, 3, 0).wait_recv()
        z_copy(c, 3, 1).wait_recv()
        for h in range(2):
            for i in range(2):
                base = [zrp[c, 3, h, i * 4 + t].astype(jnp.float32) + zrm[c, 3, h, i * 4 + t].astype(jnp.float32)
                        for t in range(4)]
                for t, v in enumerate(local_sum(c, h, z, i, base)):
                    if i == 0:
                        x2s[c, h, t] = v.astype(jnp.bfloat16)
                    else:
                        fin[c, h, t] = v
            x2_copy(c, h).start()

    def finish(c):
        for h in range(2):
            x2_copy(c, h).wait_recv()
            fin[c, h] = fin[c, h] + x2r[c, h].astype(jnp.float32)
        lanes = pl.ds(pl.multiple_of(y * LANES, LANES), LANES)
        for k in range(2):
            @pl.when(c == k)
            def _():
                for h in range(2):
                    rows = slice(k * 64 + h * HR, k * 64 + (h + 1) * HR)
                    out[:, rows, lanes] = parent[:, rows, lanes] - fin[k, h]

        for q in range(4):
            @pl.when(c == 2 + q)
            def _():
                f_copy_a(q).start()
                f_copy_b(q).start()

        for q in range(2):
            @pl.when(c == 6 + q)
            def _():
                f_copy_c(q).start()

    def first(part, carry):
        products(jnp.int32(0), part)
        return carry

    lax.fori_loop(0, 4, first, 0)
    x1_send(0)

    def tick(t, carry):
        c5 = t - 5

        @pl.when(c5 >= 0)
        def _():
            finish(c5)

        c4 = t - 4

        @pl.when(jnp.logical_and(c4 >= 0, c4 < CHUNKS))
        def _():
            z_last(c4)

        def inner(r, carry):
            s = 3 - r
            c = t - s

            @pl.when(jnp.logical_and(c >= 0, c < CHUNKS))
            def _():
                z_step(c, s)

            @pl.when(t + 1 < CHUNKS)
            def _():
                products(t + 1, r)

            return carry

        lax.fori_loop(0, 4, inner, 0)

        @pl.when(t + 1 < CHUNKS)
        def _():
            x1_send(t + 1)

        return carry

    lax.fori_loop(0, CHUNKS + 5, tick, 0)

    for q in range(4):
        rows = slice(q * HR, (q + 1) * HR)
        f_copy_a(q).wait_recv()
        lanes = pl.ds(pl.multiple_of(lax.rem(y + 3, NY) * LANES, LANES), LANES)
        out[:, rows, lanes] = parent[:, rows, lanes] - yra[q]
        f_copy_b(q).wait_recv()
        lanes = pl.ds(pl.multiple_of(lax.rem(y + 1, NY) * LANES, LANES), LANES)
        out[:, rows, lanes] = parent[:, rows, lanes] - yrb[q]
    for q in range(2):
        f_copy_c(q).wait_recv()
        for h in range(2):
            rows = slice(q * 64 + h * HR, q * 64 + (h + 1) * HR)
            lanes = pl.ds(pl.multiple_of(lax.rem(y + 2, NY) * LANES, LANES), LANES)
            out[:, rows, lanes] = parent[:, rows, lanes] - yrc[q, h]

    for h in range(2):
        for k in range(3):
            lab_copy(h, k).wait_send()
    for q in range(4):
        for side in range(2):
            y_copy(q, side).wait_send()
        f_copy_a(q).wait_send()
        f_copy_b(q).wait_send()
    for q in range(2):
        f_copy_c(q).wait_send()

    def drain(c, carry):
        for h in range(2):
            for k in range(3):
                x1_copy(c, h, k).wait_send()
            x2_copy(c, h).wait_send()
        for side in range(2):
            z_first(c, side).wait_send()
            for s in range(1, 4):
                z_copy(c, s, side).wait_send()
        return carry

    lax.fori_loop(0, CHUNKS, drain, 0)


def tables(src_block, dest_owner, target, counts):
    col = lax.axis_index("col")
    core, x = col % 2, col // (2 * NZ)
    slots = src_block.shape[1]
    live = jnp.arange(slots, dtype=jnp.int32) < counts[0]
    owner = dest_owner[:, 0]
    pair = src_block[0]
    within = pair % 10
    upper = sum((within >= k).astype(jnp.int32) for k in (1, 3, 6))
    lower = within - upper * (upper + 1) // 2
    base = (pair // 10) * 4
    owners = jnp.arange(64, dtype=jnp.int32)
    hit = owners[:, None] == owner[None, :]
    both = jnp.stack([base + upper, base + lower])
    tab = jnp.sum(jnp.where(hit[:, None, :], both[None], 0), axis=2).reshape(-1)
    shape = (2, 2, 2, NZ, 2)
    h, jj, cc, zo, i = [lax.broadcasted_iota(jnp.int32, shape, a) for a in range(5)]
    s = 1 - 2 * ((x + h) % 2)
    xo = (x + s * (jj * 2 + i - 1) + 8) % 4
    named = (xo * NZ + zo) * 2 + (cc + core) % 2
    hit = (named.reshape(-1)[:, None] == owner[None, :]) & live[None, :]
    label = jnp.sum(jnp.where(hit, target[None, :] + 1, 0), axis=1)
    return tab, jnp.broadcast_to(label[:, None], (128, LANES)).reshape(2, 4, 16, LANES)


def per_device(panels, parent, src_block, dest_owner, target, counts):
    tab, lab = tables(src_block, dest_owner, target, counts)
    vmem = pl.BlockSpec(memory_space=pltpu.VMEM)
    bf, f32, i32 = jnp.bfloat16, jnp.float32, jnp.int32
    dma = pltpu.SemaphoreType.DMA
    return pl.pallas_call(
        assemble_kernel,
        out_shape=jax.ShapeDtypeStruct((4, 128, 512), f32),
        in_specs=[pl.BlockSpec(memory_space=pltpu.SMEM), vmem, vmem, vmem],
        out_specs=vmem,
        scratch_shapes=[pltpu.VMEM((16, HR, 512), bf) for _ in range(8)] + [
            pltpu.VMEM((CHUNKS, 2, 4, 16, HR, LANES), bf),
            pltpu.VMEM((CHUNKS, 2, 3, 16, HR, LANES), bf),
            pltpu.VMEM((2, 3, 16, LANES), i32),
            pltpu.VMEM((CHUNKS, 4, 2, 8, HR, LANES), bf),
            pltpu.VMEM((CHUNKS, 4, 2, 8, HR, LANES), bf),
            pltpu.VMEM((CHUNKS, 4, 2, 8, HR, LANES), bf),
            pltpu.VMEM((CHUNKS, 4, 2, 8, HR, LANES), bf),
            pltpu.VMEM((CHUNKS, 2, 4, HR, LANES), bf),
            pltpu.VMEM((CHUNKS, 2, 4, HR, LANES), bf),
            pltpu.VMEM((CHUNKS, 2, 4, HR, LANES), f32),
            pltpu.VMEM((4, 4, HR, LANES), f32),
            pltpu.VMEM((4, 4, HR, LANES), f32),
            pltpu.VMEM((2, 2, 4, HR, LANES), f32),
            dma((4, 2)), dma((4, 2)),
            dma((2, 3)), dma((2, 3)),
            dma((CHUNKS, 2, 3)), dma((CHUNKS, 2, 3)),
            dma((CHUNKS, 4, 2)), dma((CHUNKS, 4, 2)),
            dma((CHUNKS, 2)), dma((CHUNKS, 2)),
            dma((6, 2)), dma((6, 2)),
        ],
        compiler_params=pltpu.CompilerParams(
            collective_id=0, has_side_effects=True, vmem_limit_bytes=60 * 1024 * 1024
        ),
    )(tab, panels.reshape(16, 128, 512), lab, parent)


def solution(mesh):
    placed = (
        P("col", None, "grp", None),
        P("col", "grp", None),
        P("col", None),
        P("col", None),
        P("col"),
        P("col"),
    )
    return jax.shard_map(
        per_device, mesh=mesh, in_specs=placed, out_specs=P("col", "grp", None), check_vma=False
    )
```

```python
import jax
import jax.numpy as jnp
from jax import lax
from jax.experimental import pallas as pl
from jax.experimental.pallas import tpu as pltpu
from jax.sharding import PartitionSpec as P

MESH = pl.DeviceIdType.MESH
NX, NZ, NY = 4, 8, 4
CHUNKS = 16
HR = 16
LANES = 128
EARLY_FROM, EARLY_STEP = 5, 3
EARLY = (CHUNKS - 1 - EARLY_FROM) // EARLY_STEP + 1
EARLY_GAP, LAST_GAP = 2, 2
UNROLL = 8
GROUP_TICK = (None, 1, 3, 5, 7, 8)


def is_early(c):
    return jnp.logical_and(lax.rem(c + EARLY_STEP * CHUNKS - EARLY_FROM, EARLY_STEP) == 0, c >= EARLY_FROM)


def assemble_kernel(
    counts, panels, src, dest, target, out,
    u0, u1, u2, u3, d0, d1, d2, d3,
    own_t, up_t, tabv, tab, lab, sendb, rx1, rlab, zsp, zrp, zsm, zrm, x2s, x2r, x2as, x2ar, fin, fr,
    t_sem, y_ss, y_rs, l_ss, l_rs, x1_ss, x1_rs, z_ss, z_rs, x2_ss, x2_rs, a_ss, a_rs, f_ss, f_rs,
):
    ups, downs = (u0, u1, u2, u3), (d0, d1, d2, d3)
    y = lax.axis_index("grp")
    col = lax.axis_index("col")
    core = lax.rem(col, 2)
    z = lax.rem(col // 2, NZ)
    x = col // (2 * NZ)

    def dev(yy, xx, zz, cc):
        return (lax.rem(yy + NY, NY), (lax.rem(xx + NX, NX) * NZ + lax.rem(zz + NZ, NZ)) * 2 + cc)

    sib = dev(y, x, z, 1 - core)
    s_of = [1 - 2 * lax.rem(x + h, 2) for h in range(2)]
    partner = [(dev(y, x + s, z, core), dev(y, x + s, z, 1 - core)) for s in s_of]
    second = [{dy: dev(y + dy, x - s, z, core) for dy in (-1, 0, 1)} for s in s_of]
    z_up, z_dn = dev(y, x, z + 1, core), dev(y, x, z - 1, core)
    y_side = {1: dev(y + 1, x, z, core), -1: dev(y - 1, x, z, core)}

    barrier = pltpu.get_barrier_semaphore()
    peers = [sib, partner[0][0], partner[0][1], partner[1][0], partner[1][1], z_up, z_dn, y_side[1], y_side[-1],
             second[0][1], second[0][-1], second[1][1], second[1][-1]]
    for peer in peers:
        pl.semaphore_signal(barrier, inc=1, device_id=peer, device_id_type=MESH)

    slots = src.shape[1]
    i32 = jnp.int32
    lane40, row40 = lax.broadcasted_iota(i32, (slots, slots), 1), lax.broadcasted_iota(i32, (slots, slots), 0)

    def column(line):
        return jnp.sum(jnp.where(lane40 == row40, jnp.broadcast_to(line, (slots, slots)), 0), axis=1, keepdims=True)

    def wide(v):
        return jnp.broadcast_to(v, (slots, LANES))

    pair = column(src[...])
    goal = column(target[...])
    front = sum((pair >= 10 * k).astype(i32) for k in (1, 2, 3))
    within = pair - 10 * front
    upper = sum((within >= k).astype(i32) for k in (1, 3, 6))
    lower = within - ((upper * (upper + 1)) >> 1)
    hit = wide(column(dest[...])) == lax.broadcasted_iota(i32, (slots, LANES), 1)
    live = lax.broadcasted_iota(i32, (slots, LANES), 0) < counts[0]

    def pick(value, mask):
        return jnp.sum(jnp.where(mask, wide(value), 0), axis=0, keepdims=True)

    tabv[...] = jnp.broadcast_to(pick((front * 4 + upper) * 16 + front * 4 + lower, hit), (8, LANES))
    tab_copy = pltpu.make_async_copy(tabv, tab, t_sem)
    tab_copy.start()
    label = pick(goal + 1, jnp.logical_and(hit, live))
    place = lax.broadcasted_iota(i32, (LANES, LANES), 0)
    pi, pz, pc, pj, ph = place & 1, (place >> 1) & 7, (place >> 4) & 1, (place >> 5) & 1, place >> 6
    turn = 1 - 2 * ((x + ph) & 1)
    named = (((x + turn * (pj * 2 + pi - 1) + 8) & 3) * NZ + pz) * 2 + ((pc + core) & 1)
    labels = jnp.sum(
        jnp.where(named == lax.broadcasted_iota(i32, (LANES, LANES), 1), jnp.broadcast_to(label, (LANES, LANES)), 0),
        axis=1, keepdims=True,
    )
    lab[...] = jnp.broadcast_to(labels, (LANES, LANES)).reshape(2, 4, 16, LANES)

    pl.semaphore_wait(barrier, len(peers))

    def rcopy(src, dst, ss, rs, who):
        return pltpu.make_async_remote_copy(
            src_ref=src, dst_ref=dst, send_sem=ss, recv_sem=rs, device_id=who, device_id_type=MESH
        )

    def y_copy(q, side):
        dst = (ups if side == 0 else downs)[q]
        return rcopy(panels.at[:, q * 32:(q + 1) * 32, :], dst, y_ss.at[q, side], y_rs.at[q, side],
                     y_side[-1] if side == 0 else y_side[1])

    def x1_who(h, k):
        return (sib, partner[h][0], partner[h][1])[k]

    def lab_copy(h, k):
        return rcopy(lab.at[h, k + 1], rlab.at[h, k], l_ss.at[h, k], l_rs.at[h, k], x1_who(h, k))

    def x1_copy(c, h, k):
        return rcopy(sendb.at[c, h, k + 1], rx1.at[c, h, k], x1_ss.at[c, h, k], x1_rs.at[c, h, k], x1_who(h, k))

    def z_copy(c, s, side, early):
        src, dst, who = ((zsp, zrp, z_up), (zsm, zrm, z_dn))[side]
        if s is None:
            s, h = 0, pl.ds(side, 1)
        else:
            h = pl.ds(0, 2)
        blocks = pl.ds(4, 4) if early else pl.ds(0, 8)
        return rcopy(src.at[c, s, h, blocks], dst.at[c, s, h, blocks], z_ss.at[c, s, side], z_rs.at[c, s, side], who)

    def a_copy(a, h):
        return rcopy(x2as.at[a, h], x2ar.at[a, h], a_ss.at[a, h], a_rs.at[a, h], second[h][0])

    def x2_copy(c, h, dy):
        return rcopy(x2s.at[c, h], x2r.at[c, h], x2_ss.at[c, h], x2_rs.at[c, h], second[h][dy])

    def f_copy(c, h, dy):
        return rcopy(fin.at[c, h], fr.at[c, h], f_ss.at[c, h], f_rs.at[c, h], y_side[dy])

    def turn_block(src, dst):
        def one(i, carry):
            dst[i] = src(i).T
            return carry

        lax.fori_loop(0, 16, one, 0)

    for q in range(4):
        for side in range(2):
            y_copy(q, side).start()
    for h in range(2):
        for k in range(3):
            lab_copy(h, k).start()
    turn_block(lambda i: panels[i], own_t)
    tab_copy.wait()

    def multiply(chunks, left, right):
        def one(n, carry):
            xo, zo, co = n // 16, lax.rem(n // 2, NZ), lax.rem(n, 2)
            both = tab[0, n]
            block = jnp.dot(left(both >> 4), right[both & 15], preferred_element_type=jnp.float32).astype(jnp.bfloat16)
            cc = lax.rem(co + core, 2)
            for h in range(2):
                e = lax.rem((xo - x) * s_of[h] + 9, 4)
                for k, c in enumerate(chunks):
                    r = (h * len(chunks) + k) * HR
                    sendb[c, h, (e // 2) * 2 + cc, zo * 2 + lax.rem(e, 2)] = block[r:r + HR]
            return carry

        lax.fori_loop(0, 64, one, 0, unroll=UNROLL)
        for c in chunks:
            x1_send(c)

    def group(k):
        if k == 0:
            multiply((0, 1, 2, 3), lambda i: panels[i], own_t)
        elif k < 5:
            y_copy(k - 1, 0).wait_recv()
            y_copy(k - 1, 1).wait_recv()
            multiply((2 * k + 2, 2 * k + 3), lambda i: jnp.concatenate([ups[k - 1][i], downs[k - 1][i]], axis=0), own_t)
        else:
            turn_block(lambda i: jnp.concatenate([u[i] for u in ups], axis=0), up_t)
            multiply((12, 13, 14, 15), lambda i: jnp.concatenate([d[i] for d in downs], axis=0), up_t)

    def x1_send(c):
        for h in range(2):
            for k in range(3):
                x1_copy(c, h, k).start()

    def x1_wait(c):
        @pl.when(c == 0)
        def _():
            for h in range(2):
                for k in range(3):
                    lab_copy(h, k).wait_recv()

        for h in range(2):
            for k in range(3):
                x1_copy(c, h, k).wait_recv()

    def local_sum(c, h, d, i, base):
        rows = d * 2 + i
        flip = d * 2 + (1 - i)
        blocks = [sendb[c, h, 0, rows], rx1[c, h, 0, rows], rx1[c, h, 1, flip], rx1[c, h, 2, flip]]
        labels = [lab[h, 0, pl.ds(rows, 1), :], rlab[h, 0, pl.ds(rows, 1), :],
                  rlab[h, 1, pl.ds(flip, 1), :], rlab[h, 2, pl.ds(flip, 1), :]]
        blocks = [b.astype(jnp.float32) for b in blocks]
        labels = [jnp.broadcast_to(v, (HR, LANES)) for v in labels]
        sums = []
        for t in range(4):
            total = None if base is None else base[t]
            for b, v in zip(blocks, labels):
                term = jnp.where(v == t + 1, b, 0.0)
                total = term if total is None else total + term
            sums.append(total)
        return sums

    def plus(a, b):
        return b if a is None else [u + v for u, v in zip(a, b)]

    def early_base(c, h, d):
        return [x2ar[(c - EARLY_FROM) // EARLY_STEP, h, d * 4 + t].astype(jnp.float32) for t in range(4)]

    def merge(c, s, h, d, prev, dst, early):
        for i in (1,) if early else (0, 1):
            base = early_base(c, h, d) if early else None
            if prev is not None:
                base = plus(base, [prev[c, s - 1, h, i * 4 + t].astype(jnp.float32) for t in range(4)])
            for t, v in enumerate(local_sum(c, h, d, i, base)):
                dst[c, s, h, i * 4 + t] = v.astype(jnp.bfloat16)

    def z_step(c, s, early):
        dp, dm = lax.rem(z + 4 - s, NZ), lax.rem(z + 4 + s, NZ)

        @pl.when(s == 0)
        def _():
            if early:
                for h in range(2):
                    a_copy((c - EARLY_FROM) // EARLY_STEP, h).wait_recv()
            else:
                x1_wait(c)
            merge(c, s, 0, dp, None, zsp, early)
            z_copy(c, None, 0, early).start()
            merge(c, s, 1, dm, None, zsm, early)
            z_copy(c, None, 1, early).start()

        @pl.when(s == 1)
        def _():
            z_copy(c, None, 0, early).wait_recv()
            merge(c, s, 0, dp, zrp, zsp, early)
            merge(c, s, 1, dp, None, zsp, early)
            z_copy(c, s, 0, early).start()
            z_copy(c, None, 1, early).wait_recv()
            merge(c, s, 1, dm, zrm, zsm, early)
            merge(c, s, 0, dm, None, zsm, early)
            z_copy(c, s, 1, early).start()

        @pl.when(s >= 2)
        def _():
            z_copy(c, s - 1, 0, early).wait_recv()
            for h in range(2):
                merge(c, s, h, dp, zrp, zsp, early)
            z_copy(c, s, 0, early).start()
            z_copy(c, s - 1, 1, early).wait_recv()
            for h in range(2):
                merge(c, s, h, dm, zrm, zsm, early)
            z_copy(c, s, 1, early).start()

    def places(c, fn):
        p, sub = c // 2, lax.rem(c, 2)

        def lanes(k):
            return pl.ds(pl.multiple_of(lax.rem(y + k, NY) * LANES, LANES), LANES)

        @pl.when(p < 2)
        def _():
            for h in range(2):
                fn(h, 0, h * 64 + c * HR, lanes(0))

        @pl.when(jnp.logical_and(p >= 2, p < 6))
        def _():
            for h in range(2):
                fn(h, 1 - 2 * h, (p - 2) * 32 + sub * HR, lanes(3 if h == 0 else 1))

        @pl.when(p >= 6)
        def _():
            for h in range(2):
                fn(h, -1, h * 64 + (c - 12) * HR, lanes(2))

    def z_last(c, early):
        z_copy(c, 3, 0, early).wait_recv()
        z_copy(c, 3, 1, early).wait_recv()
        for h in range(2):
            for i in (1,) if early else (0, 1):
                base = early_base(c, h, z) if early else None
                for buf in (zrp, zrm):
                    base = plus(base, [buf[c, 3, h, i * 4 + t].astype(jnp.float32) for t in range(4)])
                for t, v in enumerate(local_sum(c, h, z, i, base)):
                    if i == 0:
                        x2s[c, h, t] = v.astype(jnp.bfloat16)
                    else:
                        fin[c, h, t] = v

        def send(h, dy, row, lanes):
            if not early:
                x2_copy(c, h, dy).start()
            if dy != 0:
                f_copy(c, h, dy).start()

        places(c, send)

    def finish(c, early):
        def write(h, dy, row, lanes):
            if not early:
                x2_copy(c, h, dy).wait_recv()
            if dy != 0:
                f_copy(c, h, dy).wait_recv()
            value = (fin if dy == 0 else fr)[c, h]
            if not early:
                value = value + x2r[c, h].astype(jnp.float32)
            out[:, pl.ds(pl.multiple_of(row, HR), HR), lanes] = value

        places(c, write)

    def early_exchange(c):
        x1_wait(c)
        for h in range(2):
            def one(d, carry):
                for t, v in enumerate(local_sum(c, h, d, 0, None)):
                    x2as[(c - EARLY_FROM) // EARLY_STEP, h, d * 4 + t] = v.astype(jnp.bfloat16)
                return carry

            lax.fori_loop(0, NZ, one, 0)
            a_copy((c - EARLY_FROM) // EARLY_STEP, h).start()

    group(0)

    def within(c, early):
        inside = jnp.logical_and(c >= 0, c < CHUNKS)
        return jnp.logical_and(inside, is_early(c) if early else jnp.logical_not(is_early(c)))

    def tick(t, carry):
        @pl.when(within(t, True))
        def _():
            early_exchange(t)

        def inner(s, carry):
            for early in (False, True):
                c = t - s - EARLY_GAP * early

                @pl.when(within(c, early))
                def _():
                    z_step(c, s, early)

            return carry

        lax.fori_loop(0, 4, inner, 0)

        for early in (False, True):
            done = t - 4 - EARLY_GAP * early

            @pl.when(within(done, early))
            def _():
                z_last(done, early)

            @pl.when(within(done - LAST_GAP, early))
            def _():
                finish(done - LAST_GAP, early)

        for k in range(1, 6):
            @pl.when(t == GROUP_TICK[k])
            def _():
                group(k)

        return carry

    lax.fori_loop(0, CHUNKS + 4 + EARLY_GAP + LAST_GAP, tick, 0)

    for h in range(2):
        for k in range(3):
            lab_copy(h, k).wait_send()
        for a in range(EARLY):
            a_copy(a, h).wait_send()
    for q in range(4):
        for side in range(2):
            y_copy(q, side).wait_send()

    def drain(c, carry):
        for h in range(2):
            for k in range(3):
                x1_copy(c, h, k).wait_send()
        for early in (False, True):
            @pl.when(within(c, early))
            def _():
                for side in range(2):
                    z_copy(c, None, side, early).wait_send()
                    for s in range(1, 4):
                        z_copy(c, s, side, early).wait_send()

                def sent(h, dy, row, lanes):
                    if not early:
                        x2_copy(c, h, dy).wait_send()
                    if dy != 0:
                        f_copy(c, h, dy).wait_send()

                places(c, sent)
        return carry

    lax.fori_loop(0, CHUNKS, drain, 0)


def per_device(panels, parent, src_block, dest_owner, target, counts):
    vmem = pl.BlockSpec(memory_space=pltpu.VMEM)
    bf, f32, i32 = jnp.bfloat16, jnp.float32, jnp.int32
    dma = pltpu.SemaphoreType.DMA
    ring = (CHUNKS, 4, 2, 8, HR, LANES)
    tail = (CHUNKS, 2, 4, HR, LANES)
    sums = pl.pallas_call(
        assemble_kernel,
        out_shape=jax.ShapeDtypeStruct((4, 128, 512), f32),
        in_specs=[pl.BlockSpec(memory_space=pltpu.SMEM), vmem, vmem, vmem, vmem],
        out_specs=vmem,
        scratch_shapes=[pltpu.VMEM((16, 32, 512), bf) for _ in range(8)] + [
            pltpu.VMEM((16, 512, 128), bf),
            pltpu.VMEM((16, 512, 128), bf),
            pltpu.VMEM((8, LANES), i32),
            pltpu.SMEM((8, LANES), i32),
            pltpu.VMEM((2, 4, 16, LANES), i32),
            pltpu.VMEM((CHUNKS, 2, 4, 16, HR, LANES), bf),
            pltpu.VMEM((CHUNKS, 2, 3, 16, HR, LANES), bf),
            pltpu.VMEM((2, 3, 16, LANES), i32),
            pltpu.VMEM(ring, bf), pltpu.VMEM(ring, bf), pltpu.VMEM(ring, bf), pltpu.VMEM(ring, bf),
            pltpu.VMEM(tail, bf), pltpu.VMEM(tail, bf),
            pltpu.VMEM((EARLY, 2, 32, HR, LANES), bf), pltpu.VMEM((EARLY, 2, 32, HR, LANES), bf),
            pltpu.VMEM(tail, f32), pltpu.VMEM(tail, f32),
            dma,
            dma((4, 2)), dma((4, 2)),
            dma((2, 3)), dma((2, 3)),
            dma((CHUNKS, 2, 3)), dma((CHUNKS, 2, 3)),
            dma((CHUNKS, 4, 2)), dma((CHUNKS, 4, 2)),
            dma((CHUNKS, 2)), dma((CHUNKS, 2)),
            dma((EARLY, 2)), dma((EARLY, 2)),
            dma((CHUNKS, 2)), dma((CHUNKS, 2)),
        ],
        compiler_params=pltpu.CompilerParams(
            collective_id=0, has_side_effects=True, vmem_limit_bytes=54 * 1024 * 1024
        ),
    )(counts, panels.reshape(16, 128, 512), src_block, dest_owner.reshape(1, -1), target.reshape(1, -1))
    return parent - sums


def solution(mesh):
    placed = (
        P("col", None, "grp", None),
        P("col", "grp", None),
        P("col", None),
        P("col", None),
        P("col"),
        P("col"),
    )
    return jax.shard_map(
        per_device, mesh=mesh, in_specs=placed, out_specs=P("col", "grp", None), check_vma=False
    )
```

```python
import jax
import jax.numpy as jnp
from jax import lax
from jax.experimental import pallas as pl
from jax.experimental.pallas import tpu as pltpu
from jax.sharding import PartitionSpec as P

MESH = pl.DeviceIdType.MESH
NX, NZ, NY = 4, 8, 4
CHUNKS = 16
HR = 16
LANES = 128
EARLY_FROM, EARLY_END, EARLY_STEP = 6, 13, 3
EARLY = (EARLY_END - 1 - EARLY_FROM) // EARLY_STEP + 1
EARLY_GAP, RING, LAST_GAP = 3, 5, 4
UNROLL = 8
GROUP_AT = (None, (1, 2), (4, 2), (6, 1), (8, 2), (9, 3))


def is_early(c):
    turn = lax.rem(c + EARLY_STEP * CHUNKS - EARLY_FROM, EARLY_STEP) == 0
    return jnp.logical_and(turn, jnp.logical_and(c >= EARLY_FROM, c < EARLY_END))


def assemble_kernel(
    counts, panels, src, dest, target, out,
    u0, u1, u2, u3, d0, d1, d2, d3,
    own_t, up_t, tabv, tab, lab, sendb, rx1, rlab, zsp, zrp, zsm, zrm, x2s, x2r, x2as, x2ar, fin, fr,
    t_sem, y_ss, y_rs, l_ss, l_rs, x1_ss, x1_rs, z_ss, z_rs, x2_ss, x2_rs, a_ss, a_rs, f_ss, f_rs,
):
    ups, downs = (u0, u1, u2, u3), (d0, d1, d2, d3)
    y = lax.axis_index("grp")
    col = lax.axis_index("col")
    core = lax.rem(col, 2)
    z = lax.rem(col // 2, NZ)
    x = col // (2 * NZ)

    def dev(yy, xx, zz, cc):
        return (lax.rem(yy + NY, NY), (lax.rem(xx + NX, NX) * NZ + lax.rem(zz + NZ, NZ)) * 2 + cc)

    sib = dev(y, x, z, 1 - core)
    s_of = [1 - 2 * lax.rem(x + h, 2) for h in range(2)]
    partner = [(dev(y, x + s, z, core), dev(y, x + s, z, 1 - core)) for s in s_of]
    second = [{dy: dev(y + dy, x - s, z, core) for dy in (-1, 0, 1)} for s in s_of]
    z_up, z_dn = dev(y, x, z + 1, core), dev(y, x, z - 1, core)
    y_side = {1: dev(y + 1, x, z, core), -1: dev(y - 1, x, z, core)}

    barrier = pltpu.get_barrier_semaphore()
    peers = [sib, partner[0][0], partner[0][1], partner[1][0], partner[1][1], z_up, z_dn, y_side[1], y_side[-1],
             second[0][1], second[0][-1], second[1][1], second[1][-1]]
    for peer in peers:
        pl.semaphore_signal(barrier, inc=1, device_id=peer, device_id_type=MESH)

    slots = src.shape[1]
    i32 = jnp.int32
    lane40, row40 = lax.broadcasted_iota(i32, (slots, slots), 1), lax.broadcasted_iota(i32, (slots, slots), 0)

    def column(line):
        return jnp.sum(jnp.where(lane40 == row40, jnp.broadcast_to(line, (slots, slots)), 0), axis=1, keepdims=True)

    def wide(v):
        return jnp.broadcast_to(v, (slots, LANES))

    pair = column(src[...])
    goal = column(target[...])
    front = sum((pair >= 10 * k).astype(i32) for k in (1, 2, 3))
    within = pair - 10 * front
    upper = sum((within >= k).astype(i32) for k in (1, 3, 6))
    lower = within - ((upper * (upper + 1)) >> 1)
    hit = wide(column(dest[...])) == lax.broadcasted_iota(i32, (slots, LANES), 1)
    live = lax.broadcasted_iota(i32, (slots, LANES), 0) < counts[0]

    def pick(value, mask):
        return jnp.sum(jnp.where(mask, wide(value), 0), axis=0, keepdims=True)

    tabv[...] = jnp.broadcast_to(pick((front * 4 + upper) * 16 + front * 4 + lower, hit), (8, LANES))
    tab_copy = pltpu.make_async_copy(tabv, tab, t_sem)
    tab_copy.start()
    label = pick(goal + 1, jnp.logical_and(hit, live))
    place = lax.broadcasted_iota(i32, (LANES, LANES), 0)
    pi, pz, pc, pj, ph = place & 1, (place >> 1) & 7, (place >> 4) & 1, (place >> 5) & 1, place >> 6
    turn = 1 - 2 * ((x + ph) & 1)
    named = (((x + turn * (pj * 2 + pi - 1) + 8) & 3) * NZ + pz) * 2 + ((pc + core) & 1)
    labels = jnp.sum(
        jnp.where(named == lax.broadcasted_iota(i32, (LANES, LANES), 1), jnp.broadcast_to(label, (LANES, LANES)), 0),
        axis=1, keepdims=True,
    )
    lab[...] = jnp.broadcast_to(labels, (LANES, LANES)).reshape(2, 4, 16, LANES)

    pl.semaphore_wait(barrier, len(peers))

    def rcopy(src, dst, ss, rs, who):
        return pltpu.make_async_remote_copy(
            src_ref=src, dst_ref=dst, send_sem=ss, recv_sem=rs, device_id=who, device_id_type=MESH
        )

    def y_copy(q, side):
        dst = (ups if side == 0 else downs)[q]
        return rcopy(panels.at[:, q * 32:(q + 1) * 32, :], dst, y_ss.at[q, side], y_rs.at[q, side],
                     y_side[-1] if side == 0 else y_side[1])

    def x1_who(h, k):
        return (sib, partner[h][0], partner[h][1])[k]

    def lab_copy(h, k):
        return rcopy(lab.at[h, k + 1], rlab.at[h, k], l_ss.at[h, k], l_rs.at[h, k], x1_who(h, k))

    def x1_copy(c, h, k):
        return rcopy(sendb.at[c, h, k + 1], rx1.at[c, h, k], x1_ss.at[c, h, k], x1_rs.at[c, h, k], x1_who(h, k))

    def z_copy(c, s, side, early):
        src, dst, who = ((zsp, zrp, z_up), (zsm, zrm, z_dn))[side]
        if s is None:
            s, h = 0, pl.ds(side, 1)
        else:
            h = pl.ds(0, 2)
        blocks = pl.ds(4, 4) if early else pl.ds(0, 8)
        return rcopy(src.at[c, s, h, blocks], dst.at[c, s, h, blocks], z_ss.at[c, s, side], z_rs.at[c, s, side], who)

    def a_copy(a, h):
        return rcopy(x2as.at[a, h], x2ar.at[a, h], a_ss.at[a, h], a_rs.at[a, h], second[h][0])

    def x2_copy(c, h, dy):
        return rcopy(x2s.at[c, h], x2r.at[c, h], x2_ss.at[c, h], x2_rs.at[c, h], second[h][dy])

    def f_copy(c, h, dy):
        return rcopy(fin.at[c, h], fr.at[c, h], f_ss.at[c, h], f_rs.at[c, h], y_side[dy])

    def turn_block(src, dst):
        def one(i, carry):
            dst[i] = src(i).T
            return carry

        lax.fori_loop(0, 16, one, 0)

    for q in range(4):
        for side in range(2):
            y_copy(q, side).start()
    for h in range(2):
        for k in range(3):
            lab_copy(h, k).start()
    turn_block(lambda i: panels[i], own_t)
    tab_copy.wait()

    def multiply(chunks, left, right):
        def one(n, carry):
            xo, zo, co = n // 16, lax.rem(n // 2, NZ), lax.rem(n, 2)
            both = tab[0, n]
            block = jnp.dot(left(both >> 4), right[both & 15], preferred_element_type=jnp.float32).astype(jnp.bfloat16)
            cc = lax.rem(co + core, 2)
            for h in range(2):
                e = lax.rem((xo - x) * s_of[h] + 9, 4)
                for k, c in enumerate(chunks):
                    r = (h * len(chunks) + k) * HR
                    sendb[c, h, (e // 2) * 2 + cc, zo * 2 + lax.rem(e, 2)] = block[r:r + HR]
            return carry

        lax.fori_loop(0, 64, one, 0, unroll=UNROLL)
        for c in chunks:
            x1_send(c)

    def group(k):
        if k == 0:
            multiply((0, 1, 2, 3), lambda i: panels[i], own_t)
        elif k < 5:
            y_copy(k - 1, 0).wait_recv()
            y_copy(k - 1, 1).wait_recv()
            multiply((2 * k + 2, 2 * k + 3), lambda i: jnp.concatenate([ups[k - 1][i], downs[k - 1][i]], axis=0), own_t)
        else:
            turn_block(lambda i: jnp.concatenate([u[i] for u in ups], axis=0), up_t)
            multiply((12, 13, 14, 15), lambda i: jnp.concatenate([d[i] for d in downs], axis=0), up_t)

    def x1_send(c):
        for h in range(2):
            for k in range(3):
                x1_copy(c, h, k).start()

    def x1_wait(c):
        @pl.when(c == 0)
        def _():
            for h in range(2):
                for k in range(3):
                    lab_copy(h, k).wait_recv()

        for h in range(2):
            for k in range(3):
                x1_copy(c, h, k).wait_recv()

    def local_sum(c, h, d, i, base):
        rows = d * 2 + i
        flip = d * 2 + (1 - i)
        blocks = [sendb[c, h, 0, rows], rx1[c, h, 0, rows], rx1[c, h, 1, flip], rx1[c, h, 2, flip]]
        labels = [lab[h, 0, pl.ds(rows, 1), :], rlab[h, 0, pl.ds(rows, 1), :],
                  rlab[h, 1, pl.ds(flip, 1), :], rlab[h, 2, pl.ds(flip, 1), :]]
        blocks = [b.astype(jnp.float32) for b in blocks]
        labels = [jnp.broadcast_to(v, (HR, LANES)) for v in labels]
        sums = []
        for t in range(4):
            total = None if base is None else base[t]
            for b, v in zip(blocks, labels):
                term = jnp.where(v == t + 1, b, 0.0)
                total = term if total is None else total + term
            sums.append(total)
        return sums

    def plus(a, b):
        return b if a is None else [u + v for u, v in zip(a, b)]

    def early_base(c, h, d):
        return [x2ar[(c - EARLY_FROM) // EARLY_STEP, h, d * 4 + t].astype(jnp.float32) for t in range(4)]

    def merge(c, s, h, d, prev, dst, early):
        for i in (1,) if early else (0, 1):
            base = early_base(c, h, d) if early else None
            if prev is not None:
                base = plus(base, [prev[c, s - 1, h, i * 4 + t].astype(jnp.float32) for t in range(4)])
            for t, v in enumerate(local_sum(c, h, d, i, base)):
                dst[c, s, h, i * 4 + t] = v.astype(jnp.bfloat16)

    def z_step(c, s, early):
        dp, dm = lax.rem(z + 4 - s, NZ), lax.rem(z + 4 + s, NZ)

        @pl.when(s == 0)
        def _():
            if early:
                for h in range(2):
                    a_copy((c - EARLY_FROM) // EARLY_STEP, h).wait_recv()
            else:
                x1_wait(c)
            merge(c, s, 0, dp, None, zsp, early)
            z_copy(c, None, 0, early).start()
            merge(c, s, 1, dm, None, zsm, early)
            z_copy(c, None, 1, early).start()

        @pl.when(s == 1)
        def _():
            z_copy(c, None, 0, early).wait_recv()
            merge(c, s, 0, dp, zrp, zsp, early)
            merge(c, s, 1, dp, None, zsp, early)
            z_copy(c, s, 0, early).start()
            z_copy(c, None, 1, early).wait_recv()
            merge(c, s, 1, dm, zrm, zsm, early)
            merge(c, s, 0, dm, None, zsm, early)
            z_copy(c, s, 1, early).start()

        @pl.when(s >= 2)
        def _():
            z_copy(c, s - 1, 0, early).wait_recv()
            for h in range(2):
                merge(c, s, h, dp, zrp, zsp, early)
            z_copy(c, s, 0, early).start()
            z_copy(c, s - 1, 1, early).wait_recv()
            for h in range(2):
                merge(c, s, h, dm, zrm, zsm, early)
            z_copy(c, s, 1, early).start()

    def places(c, fn):
        p, sub = c // 2, lax.rem(c, 2)

        def lanes(k):
            return pl.ds(pl.multiple_of(lax.rem(y + k, NY) * LANES, LANES), LANES)

        @pl.when(p < 2)
        def _():
            for h in range(2):
                fn(h, 0, h * 64 + c * HR, lanes(0))

        @pl.when(jnp.logical_and(p >= 2, p < 6))
        def _():
            for h in range(2):
                fn(h, 1 - 2 * h, (p - 2) * 32 + sub * HR, lanes(3 if h == 0 else 1))

        @pl.when(p >= 6)
        def _():
            for h in range(2):
                fn(h, -1, h * 64 + (c - 12) * HR, lanes(2))

    def z_last(c, early):
        z_copy(c, 3, 0, early).wait_recv()
        z_copy(c, 3, 1, early).wait_recv()
        for h in range(2):
            for i in (1,) if early else (0, 1):
                base = early_base(c, h, z) if early else None
                for buf in (zrp, zrm):
                    base = plus(base, [buf[c, 3, h, i * 4 + t].astype(jnp.float32) for t in range(4)])
                for t, v in enumerate(local_sum(c, h, z, i, base)):
                    if i == 0:
                        x2s[c, h, t] = v.astype(jnp.bfloat16)
                    else:
                        fin[c, h, t] = v

        def send(h, dy, row, lanes):
            if not early:
                x2_copy(c, h, dy).start()
            if dy != 0:
                f_copy(c, h, dy).start()

        places(c, send)

    def finish(c, early):
        def write(h, dy, row, lanes):
            if not early:
                x2_copy(c, h, dy).wait_recv()
            if dy != 0:
                f_copy(c, h, dy).wait_recv()
            value = (fin if dy == 0 else fr)[c, h]
            if not early:
                value = value + x2r[c, h].astype(jnp.float32)
            out[:, pl.ds(pl.multiple_of(row, HR), HR), lanes] = value

        places(c, write)

    def early_exchange(c):
        x1_wait(c)
        for h in range(2):
            def one(d, carry):
                for t, v in enumerate(local_sum(c, h, d, 0, None)):
                    x2as[(c - EARLY_FROM) // EARLY_STEP, h, d * 4 + t] = v.astype(jnp.bfloat16)
                return carry

            lax.fori_loop(0, NZ, one, 0)
            a_copy((c - EARLY_FROM) // EARLY_STEP, h).start()

    group(0)

    def within(c, early):
        inside = jnp.logical_and(c >= 0, c < CHUNKS)
        return jnp.logical_and(inside, is_early(c) if early else jnp.logical_not(is_early(c)))

    def tick(t, carry):
        @pl.when(within(t, True))
        def _():
            early_exchange(t)

        def inner(s, carry):
            for early in (False, True):
                c = t - s - EARLY_GAP * early

                @pl.when(within(c, early))
                def _():
                    z_step(c, s, early)

            for k in range(1, 6):
                @pl.when(jnp.logical_and(t == GROUP_AT[k][0], s == GROUP_AT[k][1]))
                def _():
                    group(k)

            return carry

        lax.fori_loop(0, 4, inner, 0)

        for early in (False, True):
            done = t - RING - EARLY_GAP * early

            @pl.when(within(done, early))
            def _():
                z_last(done, early)

            @pl.when(within(done - LAST_GAP, early))
            def _():
                finish(done - LAST_GAP, early)

        return carry

    lax.fori_loop(0, CHUNKS + RING + EARLY_GAP + LAST_GAP, tick, 0)

    for h in range(2):
        for k in range(3):
            lab_copy(h, k).wait_send()
        for a in range(EARLY):
            a_copy(a, h).wait_send()
    for q in range(4):
        for side in range(2):
            y_copy(q, side).wait_send()

    def drain(c, carry):
        for h in range(2):
            for k in range(3):
                x1_copy(c, h, k).wait_send()
        for early in (False, True):
            @pl.when(within(c, early))
            def _():
                for side in range(2):
                    z_copy(c, None, side, early).wait_send()
                    for s in range(1, 4):
                        z_copy(c, s, side, early).wait_send()

                def sent(h, dy, row, lanes):
                    if not early:
                        x2_copy(c, h, dy).wait_send()
                    if dy != 0:
                        f_copy(c, h, dy).wait_send()

                places(c, sent)
        return carry

    lax.fori_loop(0, CHUNKS, drain, 0)


def per_device(panels, parent, src_block, dest_owner, target, counts):
    vmem = pl.BlockSpec(memory_space=pltpu.VMEM)
    bf, f32, i32 = jnp.bfloat16, jnp.float32, jnp.int32
    dma = pltpu.SemaphoreType.DMA
    ring = (CHUNKS, 4, 2, 8, HR, LANES)
    tail = (CHUNKS, 2, 4, HR, LANES)
    sums = pl.pallas_call(
        assemble_kernel,
        out_shape=jax.ShapeDtypeStruct((4, 128, 512), f32),
        in_specs=[pl.BlockSpec(memory_space=pltpu.SMEM), vmem, vmem, vmem, vmem],
        out_specs=vmem,
        scratch_shapes=[pltpu.VMEM((16, 32, 512), bf) for _ in range(8)] + [
            pltpu.VMEM((16, 512, 128), bf),
            pltpu.VMEM((16, 512, 128), bf),
            pltpu.VMEM((8, LANES), i32),
            pltpu.SMEM((8, LANES), i32),
            pltpu.VMEM((2, 4, 16, LANES), i32),
            pltpu.VMEM((CHUNKS, 2, 4, 16, HR, LANES), bf),
            pltpu.VMEM((CHUNKS, 2, 3, 16, HR, LANES), bf),
            pltpu.VMEM((2, 3, 16, LANES), i32),
            pltpu.VMEM(ring, bf), pltpu.VMEM(ring, bf), pltpu.VMEM(ring, bf), pltpu.VMEM(ring, bf),
            pltpu.VMEM(tail, bf), pltpu.VMEM(tail, bf),
            pltpu.VMEM((EARLY, 2, 32, HR, LANES), bf), pltpu.VMEM((EARLY, 2, 32, HR, LANES), bf),
            pltpu.VMEM(tail, f32), pltpu.VMEM(tail, f32),
            dma,
            dma((4, 2)), dma((4, 2)),
            dma((2, 3)), dma((2, 3)),
            dma((CHUNKS, 2, 3)), dma((CHUNKS, 2, 3)),
            dma((CHUNKS, 4, 2)), dma((CHUNKS, 4, 2)),
            dma((CHUNKS, 2)), dma((CHUNKS, 2)),
            dma((EARLY, 2)), dma((EARLY, 2)),
            dma((CHUNKS, 2)), dma((CHUNKS, 2)),
        ],
        compiler_params=pltpu.CompilerParams(
            collective_id=0, has_side_effects=True, vmem_limit_bytes=49 * 1024 * 1024
        ),
    )(counts, panels.reshape(16, 128, 512), src_block, dest_owner.reshape(1, -1), target.reshape(1, -1))
    return parent - sums


def solution(mesh):
    placed = (
        P("col", None, "grp", None),
        P("col", "grp", None),
        P("col", None),
        P("col", None),
        P("col"),
        P("col"),
    )
    return jax.shard_map(
        per_device, mesh=mesh, in_specs=placed, out_specs=P("col", "grp", None), check_vma=False
    )
```

```python
import jax
import jax.numpy as jnp
from jax import lax
from jax.experimental import pallas as pl
from jax.experimental.pallas import tpu as pltpu
from jax.sharding import PartitionSpec as P

MESH = pl.DeviceIdType.MESH
NX, NZ, NY = 4, 8, 4
CHUNKS = 16
HR = 16
LANES = 128
EARLY_FROM, EARLY_END, EARLY_STEP = 6, 13, 3
EARLY = (EARLY_END - 1 - EARLY_FROM) // EARLY_STEP + 1
EARLY_GAP, RING, LAST_GAP = 2, 4, 4
UNROLL = 8
GROUP_AT = (None, (1, 2), (4, 2), (6, 1), (8, 2), (9, 3))


def is_early(c):
    turn = lax.rem(c + EARLY_STEP * CHUNKS - EARLY_FROM, EARLY_STEP) == 0
    return jnp.logical_and(turn, jnp.logical_and(c >= EARLY_FROM, c < EARLY_END))


def assemble_kernel(
    counts, panels, src, dest, target, out,
    u0, u1, u2, u3, d0, d1, d2, d3,
    own_t, up_t, tabv, tab, lab, sendb, rx1, rlab, zsp, zrp, zsm, zrm, x2s, x2r, x2as, x2ar, fin, fr,
    t_sem, y_ss, y_rs, l_ss, l_rs, x1_ss, x1_rs, z_ss, z_rs, x2_ss, x2_rs, a_ss, a_rs, f_ss, f_rs,
):
    ups, downs = (u0, u1, u2, u3), (d0, d1, d2, d3)
    y = lax.axis_index("grp")
    col = lax.axis_index("col")
    core = lax.rem(col, 2)
    z = lax.rem(col // 2, NZ)
    x = col // (2 * NZ)

    def dev(yy, xx, zz, cc):
        return (lax.rem(yy + NY, NY), (lax.rem(xx + NX, NX) * NZ + lax.rem(zz + NZ, NZ)) * 2 + cc)

    sib = dev(y, x, z, 1 - core)
    s_of = [1 - 2 * lax.rem(x + h, 2) for h in range(2)]
    partner = [(dev(y, x + s, z, core), dev(y, x + s, z, 1 - core)) for s in s_of]
    second = [{dy: dev(y + dy, x - s, z, core) for dy in (-1, 0, 1)} for s in s_of]
    z_up, z_dn = dev(y, x, z + 1, core), dev(y, x, z - 1, core)
    y_side = {1: dev(y + 1, x, z, core), -1: dev(y - 1, x, z, core)}

    barrier = pltpu.get_barrier_semaphore()
    peers = [sib, partner[0][0], partner[0][1], partner[1][0], partner[1][1], z_up, z_dn, y_side[1], y_side[-1],
             second[0][1], second[0][-1], second[1][1], second[1][-1]]
    for peer in peers:
        pl.semaphore_signal(barrier, inc=1, device_id=peer, device_id_type=MESH)

    pl.semaphore_wait(barrier, len(peers))

    def rcopy(src, dst, ss, rs, who):
        return pltpu.make_async_remote_copy(
            src_ref=src, dst_ref=dst, send_sem=ss, recv_sem=rs, device_id=who, device_id_type=MESH
        )

    def y_copy(q, side):
        dst = (ups if side == 0 else downs)[q]
        return rcopy(panels.at[:, q * 32:(q + 1) * 32, :], dst, y_ss.at[q, side], y_rs.at[q, side],
                     y_side[-1] if side == 0 else y_side[1])

    for q in range(4):
        for side in range(2):
            y_copy(q, side).start()

    slots = src.shape[1]
    i32 = jnp.int32
    lane40, row40 = lax.broadcasted_iota(i32, (slots, slots), 1), lax.broadcasted_iota(i32, (slots, slots), 0)

    def column(line):
        return jnp.sum(jnp.where(lane40 == row40, jnp.broadcast_to(line, (slots, slots)), 0), axis=1, keepdims=True)

    def wide(v):
        return jnp.broadcast_to(v, (slots, LANES))

    pair = column(src[...])
    goal = column(target[...])
    front = sum((pair >= 10 * k).astype(i32) for k in (1, 2, 3))
    within = pair - 10 * front
    upper = sum((within >= k).astype(i32) for k in (1, 3, 6))
    lower = within - ((upper * (upper + 1)) >> 1)
    hit = wide(column(dest[...])) == lax.broadcasted_iota(i32, (slots, LANES), 1)
    live = lax.broadcasted_iota(i32, (slots, LANES), 0) < counts[0]

    def pick(value, mask):
        return jnp.sum(jnp.where(mask, wide(value), 0), axis=0, keepdims=True)

    tabv[...] = jnp.broadcast_to(pick((front * 4 + upper) * 16 + front * 4 + lower, hit), (8, LANES))
    tab_copy = pltpu.make_async_copy(tabv, tab, t_sem)
    tab_copy.start()
    label = pick(goal + 1, jnp.logical_and(hit, live))
    place = lax.broadcasted_iota(i32, (LANES, LANES), 0)
    pi, pz, pc, pj, ph = place & 1, (place >> 1) & 7, (place >> 4) & 1, (place >> 5) & 1, place >> 6
    turn = 1 - 2 * ((x + ph) & 1)
    named = (((x + turn * (pj * 2 + pi - 1) + 8) & 3) * NZ + pz) * 2 + ((pc + core) & 1)
    labels = jnp.sum(
        jnp.where(named == lax.broadcasted_iota(i32, (LANES, LANES), 1), jnp.broadcast_to(label, (LANES, LANES)), 0),
        axis=1, keepdims=True,
    )
    lab[...] = jnp.broadcast_to(labels, (LANES, LANES)).reshape(2, 4, 16, LANES)


    def x1_who(h, k):
        return (sib, partner[h][0], partner[h][1])[k]

    def lab_copy(h, k):
        return rcopy(lab.at[h, k + 1], rlab.at[h, k], l_ss.at[h, k], l_rs.at[h, k], x1_who(h, k))

    def x1_copy(c, h, k):
        return rcopy(sendb.at[c, h, k + 1], rx1.at[c, h, k], x1_ss.at[c, h, k], x1_rs.at[c, h, k], x1_who(h, k))

    def z_copy(c, s, side, early):
        src, dst, who = ((zsp, zrp, z_up), (zsm, zrm, z_dn))[side]
        if s is None:
            s, h = 0, pl.ds(side, 1)
        else:
            h = pl.ds(0, 2)
        blocks = pl.ds(4, 4) if early else pl.ds(0, 8)
        return rcopy(src.at[c, s, h, blocks], dst.at[c, s, h, blocks], z_ss.at[c, s, side], z_rs.at[c, s, side], who)

    def a_copy(a, h):
        return rcopy(x2as.at[a, h], x2ar.at[a, h], a_ss.at[a, h], a_rs.at[a, h], second[h][0])

    def x2_copy(c, h, dy):
        return rcopy(x2s.at[c, h], x2r.at[c, h], x2_ss.at[c, h], x2_rs.at[c, h], second[h][dy])

    def f_copy(c, h, dy):
        return rcopy(fin.at[c, h], fr.at[c, h], f_ss.at[c, h], f_rs.at[c, h], y_side[dy])

    def turn_block(src, dst):
        def one(i, carry):
            dst[i] = src(i).T
            return carry

        lax.fori_loop(0, 16, one, 0)

    for h in range(2):
        for k in range(3):
            lab_copy(h, k).start()
    turn_block(lambda i: panels[i], own_t)
    tab_copy.wait()

    def multiply(chunks, left, right):
        def one(n, carry):
            xo, zo, co = n // 16, lax.rem(n // 2, NZ), lax.rem(n, 2)
            both = tab[0, n]
            block = jnp.dot(left(both >> 4), right[both & 15], preferred_element_type=jnp.float32).astype(jnp.bfloat16)
            cc = lax.rem(co + core, 2)
            for h in range(2):
                e = lax.rem((xo - x) * s_of[h] + 9, 4)
                for k, c in enumerate(chunks):
                    r = (h * len(chunks) + k) * HR
                    sendb[c, h, (e // 2) * 2 + cc, zo * 2 + lax.rem(e, 2)] = block[r:r + HR]
            return carry

        lax.fori_loop(0, 64, one, 0, unroll=UNROLL)
        for c in chunks:
            x1_send(c)

    def group(k):
        if k == 0:
            multiply((0, 1, 2, 3), lambda i: panels[i], own_t)
        elif k < 5:
            y_copy(k - 1, 0).wait_recv()
            y_copy(k - 1, 1).wait_recv()
            multiply((2 * k + 2, 2 * k + 3), lambda i: jnp.concatenate([ups[k - 1][i], downs[k - 1][i]], axis=0), own_t)
        else:
            turn_block(lambda i: jnp.concatenate([u[i] for u in ups], axis=0), up_t)
            multiply((12, 13, 14, 15), lambda i: jnp.concatenate([d[i] for d in downs], axis=0), up_t)

    def x1_send(c):
        for h in range(2):
            for k in range(3):
                x1_copy(c, h, k).start()

    def x1_wait(c):
        @pl.when(c == 0)
        def _():
            for h in range(2):
                for k in range(3):
                    lab_copy(h, k).wait_recv()

        for h in range(2):
            for k in range(3):
                x1_copy(c, h, k).wait_recv()

    def local_sum(c, h, d, i, base):
        rows = d * 2 + i
        flip = d * 2 + (1 - i)
        blocks = [sendb[c, h, 0, rows], rx1[c, h, 0, rows], rx1[c, h, 1, flip], rx1[c, h, 2, flip]]
        labels = [lab[h, 0, pl.ds(rows, 1), :], rlab[h, 0, pl.ds(rows, 1), :],
                  rlab[h, 1, pl.ds(flip, 1), :], rlab[h, 2, pl.ds(flip, 1), :]]
        blocks = [b.astype(jnp.float32) for b in blocks]
        labels = [jnp.broadcast_to(v, (HR, LANES)) for v in labels]
        sums = []
        for t in range(4):
            total = None if base is None else base[t]
            for b, v in zip(blocks, labels):
                term = jnp.where(v == t + 1, b, 0.0)
                total = term if total is None else total + term
            sums.append(total)
        return sums

    def plus(a, b):
        return b if a is None else [u + v for u, v in zip(a, b)]

    def early_base(c, h, d):
        return [x2ar[(c - EARLY_FROM) // EARLY_STEP, h, d * 4 + t].astype(jnp.float32) for t in range(4)]

    def merge(c, s, h, d, prev, dst, early):
        for i in (1,) if early else (0, 1):
            base = early_base(c, h, d) if early else None
            if prev is not None:
                base = plus(base, [prev[c, s - 1, h, i * 4 + t].astype(jnp.float32) for t in range(4)])
            for t, v in enumerate(local_sum(c, h, d, i, base)):
                dst[c, s, h, i * 4 + t] = v.astype(jnp.bfloat16)

    def z_step(c, s, early):
        dp, dm = lax.rem(z + 4 - s, NZ), lax.rem(z + 4 + s, NZ)

        @pl.when(s == 0)
        def _():
            if early:
                for h in range(2):
                    a_copy((c - EARLY_FROM) // EARLY_STEP, h).wait_recv()
            else:
                x1_wait(c)
            merge(c, s, 0, dp, None, zsp, early)
            z_copy(c, None, 0, early).start()
            merge(c, s, 1, dm, None, zsm, early)
            z_copy(c, None, 1, early).start()

        @pl.when(s == 1)
        def _():
            z_copy(c, None, 0, early).wait_recv()
            merge(c, s, 0, dp, zrp, zsp, early)
            merge(c, s, 1, dp, None, zsp, early)
            z_copy(c, s, 0, early).start()
            z_copy(c, None, 1, early).wait_recv()
            merge(c, s, 1, dm, zrm, zsm, early)
            merge(c, s, 0, dm, None, zsm, early)
            z_copy(c, s, 1, early).start()

        @pl.when(s >= 2)
        def _():
            z_copy(c, s - 1, 0, early).wait_recv()
            for h in range(2):
                merge(c, s, h, dp, zrp, zsp, early)
            z_copy(c, s, 0, early).start()
            z_copy(c, s - 1, 1, early).wait_recv()
            for h in range(2):
                merge(c, s, h, dm, zrm, zsm, early)
            z_copy(c, s, 1, early).start()

    def places(c, fn):
        p, sub = c // 2, lax.rem(c, 2)

        def lanes(k):
            return pl.ds(pl.multiple_of(lax.rem(y + k, NY) * LANES, LANES), LANES)

        @pl.when(p < 2)
        def _():
            for h in range(2):
                fn(h, 0, h * 64 + c * HR, lanes(0))

        @pl.when(jnp.logical_and(p >= 2, p < 6))
        def _():
            for h in range(2):
                fn(h, 1 - 2 * h, (p - 2) * 32 + sub * HR, lanes(3 if h == 0 else 1))

        @pl.when(p >= 6)
        def _():
            for h in range(2):
                fn(h, -1, h * 64 + (c - 12) * HR, lanes(2))

    def z_last(c, early):
        z_copy(c, 3, 0, early).wait_recv()
        z_copy(c, 3, 1, early).wait_recv()
        for h in range(2):
            for i in (1,) if early else (0, 1):
                base = early_base(c, h, z) if early else None
                for buf in (zrp, zrm):
                    base = plus(base, [buf[c, 3, h, i * 4 + t].astype(jnp.float32) for t in range(4)])
                for t, v in enumerate(local_sum(c, h, z, i, base)):
                    if i == 0:
                        x2s[c, h, t] = v.astype(jnp.bfloat16)
                    else:
                        fin[c, h, t] = v

        def send(h, dy, row, lanes):
            if not early:
                x2_copy(c, h, dy).start()
            if dy != 0:
                f_copy(c, h, dy).start()

        places(c, send)

    def finish(c, early):
        def write(h, dy, row, lanes):
            if not early:
                x2_copy(c, h, dy).wait_recv()
            if dy != 0:
                f_copy(c, h, dy).wait_recv()
            value = (fin if dy == 0 else fr)[c, h]
            if not early:
                value = value + x2r[c, h].astype(jnp.float32)
            out[:, pl.ds(pl.multiple_of(row, HR), HR), lanes] = value

        places(c, write)

    def early_exchange(c):
        x1_wait(c)
        for h in range(2):
            def one(d, carry):
                for t, v in enumerate(local_sum(c, h, d, 0, None)):
                    x2as[(c - EARLY_FROM) // EARLY_STEP, h, d * 4 + t] = v.astype(jnp.bfloat16)
                return carry

            lax.fori_loop(0, NZ, one, 0)
            a_copy((c - EARLY_FROM) // EARLY_STEP, h).start()

    group(0)

    def within(c, early):
        inside = jnp.logical_and(c >= 0, c < CHUNKS)
        return jnp.logical_and(inside, is_early(c) if early else jnp.logical_not(is_early(c)))

    def tick(t, carry):
        @pl.when(within(t, True))
        def _():
            early_exchange(t)

        def inner(s, carry):
            for early in (False, True):
                c = t - s - EARLY_GAP * early

                @pl.when(within(c, early))
                def _():
                    z_step(c, s, early)

            for k in range(1, 6):
                @pl.when(jnp.logical_and(t == GROUP_AT[k][0], s == GROUP_AT[k][1]))
                def _():
                    group(k)

            return carry

        lax.fori_loop(0, 4, inner, 0)

        for early in (False, True):
            done = t - RING - EARLY_GAP * early

            @pl.when(within(done, early))
            def _():
                z_last(done, early)

            @pl.when(within(done - LAST_GAP, early))
            def _():
                finish(done - LAST_GAP, early)

        return carry

    lax.fori_loop(0, CHUNKS + RING + EARLY_GAP + LAST_GAP, tick, 0)

    for h in range(2):
        for k in range(3):
            lab_copy(h, k).wait_send()
        for a in range(EARLY):
            a_copy(a, h).wait_send()
    for q in range(4):
        for side in range(2):
            y_copy(q, side).wait_send()

    def drain(c, carry):
        for h in range(2):
            for k in range(3):
                x1_copy(c, h, k).wait_send()
        for early in (False, True):
            @pl.when(within(c, early))
            def _():
                for side in range(2):
                    z_copy(c, None, side, early).wait_send()
                    for s in range(1, 4):
                        z_copy(c, s, side, early).wait_send()

                def sent(h, dy, row, lanes):
                    if not early:
                        x2_copy(c, h, dy).wait_send()
                    if dy != 0:
                        f_copy(c, h, dy).wait_send()

                places(c, sent)
        return carry

    lax.fori_loop(0, CHUNKS, drain, 0)


def per_device(panels, parent, src_block, dest_owner, target, counts):
    vmem = pl.BlockSpec(memory_space=pltpu.VMEM)
    bf, f32, i32 = jnp.bfloat16, jnp.float32, jnp.int32
    dma = pltpu.SemaphoreType.DMA
    ring = (CHUNKS, 4, 2, 8, HR, LANES)
    tail = (CHUNKS, 2, 4, HR, LANES)
    sums = pl.pallas_call(
        assemble_kernel,
        out_shape=jax.ShapeDtypeStruct((4, 128, 512), f32),
        in_specs=[pl.BlockSpec(memory_space=pltpu.SMEM), vmem, vmem, vmem, vmem],
        out_specs=vmem,
        scratch_shapes=[pltpu.VMEM((16, 32, 512), bf) for _ in range(8)] + [
            pltpu.VMEM((16, 512, 128), bf),
            pltpu.VMEM((16, 512, 128), bf),
            pltpu.VMEM((8, LANES), i32),
            pltpu.SMEM((8, LANES), i32),
            pltpu.VMEM((2, 4, 16, LANES), i32),
            pltpu.VMEM((CHUNKS, 2, 4, 16, HR, LANES), bf),
            pltpu.VMEM((CHUNKS, 2, 3, 16, HR, LANES), bf),
            pltpu.VMEM((2, 3, 16, LANES), i32),
            pltpu.VMEM(ring, bf), pltpu.VMEM(ring, bf), pltpu.VMEM(ring, bf), pltpu.VMEM(ring, bf),
            pltpu.VMEM(tail, bf), pltpu.VMEM(tail, bf),
            pltpu.VMEM((EARLY, 2, 32, HR, LANES), bf), pltpu.VMEM((EARLY, 2, 32, HR, LANES), bf),
            pltpu.VMEM(tail, f32), pltpu.VMEM(tail, f32),
            dma,
            dma((4, 2)), dma((4, 2)),
            dma((2, 3)), dma((2, 3)),
            dma((CHUNKS, 2, 3)), dma((CHUNKS, 2, 3)),
            dma((CHUNKS, 4, 2)), dma((CHUNKS, 4, 2)),
            dma((CHUNKS, 2)), dma((CHUNKS, 2)),
            dma((EARLY, 2)), dma((EARLY, 2)),
            dma((CHUNKS, 2)), dma((CHUNKS, 2)),
        ],
        compiler_params=pltpu.CompilerParams(
            collective_id=0, has_side_effects=True, vmem_limit_bytes=49 * 1024 * 1024
        ),
    )(counts, panels.reshape(16, 128, 512), src_block, dest_owner.reshape(1, -1), target.reshape(1, -1))
    return parent - sums


def solution(mesh):
    placed = (
        P("col", None, "grp", None),
        P("col", "grp", None),
        P("col", None),
        P("col", None),
        P("col"),
        P("col"),
    )
    return jax.shard_map(
        per_device, mesh=mesh, in_specs=placed, out_specs=P("col", "grp", None), check_vma=False
    )
```
